32 devices in a mesh: rows: 8 (over z, y), tp: 4 (over x, core).
Axes of the slice: x: 2, y: 2, z: 4, core: 2. Of those that a mesh axis runs over, the one named last changes fastest.
Arguments:
- train_gate: float32 [3072, 8192], P('rows', 'tp'), may hold values from -0.15625 to 0.15625
- drift_gate: float32 [3072, 8192], P('rows', 'tp'), may hold values from -0.109375 to 0.109375
- spread_gate: float32 [3072, 8192], P('rows', 'tp'), may hold values from -0.109375 to 0.109375
- train_up: float32 [3072, 8192], P('rows', 'tp'), may hold values from -0.15625 to 0.15625
- drift_up: float32 [3072, 8192], P('rows', 'tp'), may hold values from -0.109375 to 0.109375
- spread_up: float32 [3072, 8192], P('rows', 'tp'), may hold values from -0.109375 to 0.109375
- norm_train: float32 [3072], P(('rows', 'tp')), may hold values from 0.25 to 1.75
- norm_step: float32 [3072], P(('rows', 'tp')), may hold values from -0.3 to 0.3
Outputs:
- serving_gate: bfloat16 [3072, 8192], P(None, 'tp')
- serving_up: bfloat16 [3072, 8192], P(None, 'tp')
- factor_gate: float32 [8192], P('tp')
- factor_up: float32 [8192], P('tp')
- serve_norm: bfloat16 [3072], replicated
- whole_gate: float32 [3072, 8192], P('rows', 'tp')
- whole_up: float32 [3072, 8192], P('rows', 'tp')
The draws below stay inside these ranges and needn't reach their ends.
All inputs are finite; a program needn't handle non-finite values.
Results may differ from the reference program's by a relative error of at most 0.001.
Values may be sent and summed in bfloat16 or wider, within the bound.
A program may use at most 128 MiB of HBM per device.

```python
import jax
import jax.numpy as jnp

D_MODEL = 3072
D_INNER = 8192


def spiked(values, rng, source, target, shards_of, factor):
    owner, partner = [(jnp.arange(values.shape[axis_at]) // (values.shape[axis_at] // shards_of)).reshape([-1 if axis == axis_at else 1 for axis in range(values.ndim)]) for axis_at in (source, target)]
    chosen = jax.random.permutation(rng, shards_of)[partner]
    strong = (owner == chosen) | (owner == (partner + shards_of // 2) % shards_of)
    return jnp.where(strong, factor * values, values)


def block_scale(stream_key, dims, cuts, low, largest):
    loudness, own = 1.0, jax.random.fold_in(stream_key, 6)
    for axis_at, parts in cuts:
        steps = jnp.exp(jax.random.uniform(jax.random.fold_in(own, axis_at), (parts,), jnp.float32, low / len(cuts), largest / len(cuts)))
        loudness = loudness * jnp.repeat(steps, dims[axis_at] // parts).reshape([-1 if axis == axis_at else 1 for axis in range(len(dims))])
    return loudness


def bell_draw(stream_key, extent, spread, most, shards=(), kind=jnp.bfloat16):
    loudness = block_scale(stream_key, extent, shards, -0.22, 0.18) if shards else 1.0
    array = jax.random.normal(stream_key, extent, jnp.float32) * spread * loudness
    return jnp.minimum(jnp.maximum(array, -most), most).astype(kind)


def heavy_noise(stream_key, dims, spread, most, split, heavy, kind=jnp.bfloat16):
    array = spread * jax.random.normal(stream_key, dims, jnp.float32)
    if split:
        array = array * block_scale(stream_key, dims, split, -0.22, 0.18)
    return jnp.clip(spiked(array, jax.random.fold_in(stream_key, 3), *heavy), -most, most).astype(kind)


def setup_inputs(seed: int = 0) -> dict:
    key_of = jax.random.split(jax.random.key(seed), 9)
    train_gate = heavy_noise(key_of[0], (D_MODEL, D_INNER), D_MODEL ** -0.5, 0.15625, ((0, 8), (1, 4)), (0, 1, 8, 2.0), jnp.float32)
    drift_gate = bell_draw(key_of[1], (D_MODEL, D_INNER), D_MODEL ** -0.5, 0.109375, ((0, 8), (1, 4)), jnp.float32)
    spread_gate = bell_draw(key_of[2], (D_MODEL, D_INNER), D_MODEL ** -0.5, 0.109375, ((0, 8), (1, 4)), jnp.float32)
    train_up = heavy_noise(key_of[3], (D_MODEL, D_INNER), D_MODEL ** -0.5, 0.15625, ((0, 8), (1, 4)), (0, 1, 8, 2.0), jnp.float32)
    drift_up = bell_draw(key_of[4], (D_MODEL, D_INNER), D_MODEL ** -0.5, 0.109375, ((0, 8), (1, 4)), jnp.float32)
    spread_up = bell_draw(key_of[5], (D_MODEL, D_INNER), D_MODEL ** -0.5, 0.109375, ((0, 8), (1, 4)), jnp.float32)
    norm_train = jnp.clip(1.0 + 0.15 * jax.random.normal(key_of[6], (D_MODEL,), jnp.float32), 0.25, 1.75)
    norm_step = jnp.clip(jax.random.uniform(key_of[7], (D_MODEL,), jnp.float32, -0.3, 0.3) * block_scale(key_of[7], (D_MODEL,), ((0, 32),), -0.4, 0.0), -0.3, 0.3)
    return dict(train_gate=train_gate, drift_gate=drift_gate, spread_gate=spread_gate, train_up=train_up, drift_up=drift_up, spread_up=spread_up, norm_train=norm_train, norm_step=norm_step)


learn_rate = 0.3
hold_rate = 0.9


def reference(train_gate, drift_gate, spread_gate, train_up, drift_up, spread_up, norm_train, norm_step):
    hold_gate = hold_rate * drift_gate + spread_gate
    whole_gate = train_gate - learn_rate * hold_gate
    hold_up = hold_rate * drift_up + spread_up
    whole_up = train_up - learn_rate * hold_up
    factor_gate = jnp.sum(jnp.abs(whole_gate), axis=0) / D_MODEL
    serving_gate = (whole_gate / factor_gate).astype(jnp.bfloat16)
    factor_up = jnp.sum(jnp.abs(whole_up), axis=0) / D_MODEL
    serving_up = (whole_up / factor_up).astype(jnp.bfloat16)
    serve_norm = (norm_train + norm_step).astype(jnp.bfloat16)
    return serving_gate, serving_up, factor_gate, factor_up, serve_norm, whole_gate, whole_up
```

```python
import jax
import jax.numpy as jnp
import numpy as np
from jax import lax
from jax.experimental import pallas as pl
from jax.experimental.pallas import tpu as pltpu
from jax.sharding import PartitionSpec as P


learn_rate = 0.3
hold_rate = 0.9


def cycle_of(mesh):
    count = mesh.shape["rows"]
    try:
        spots = [tuple(d.coords[1:]) for d in np.asarray(mesh.devices)[:, 0]]
    except (AttributeError, TypeError):
        return list(range(count))
    ys = sorted({s[0] for s in spots})
    zs = sorted({s[1] for s in spots})
    at = {s: i for i, s in enumerate(spots)}
    if len(at) != count or len(ys) * len(zs) != count:
        return list(range(count))
    if len(zs) % 2 and len(ys) % 2 == 0:
        ys, zs = zs, ys
        at = {(b, a): i for (a, b), i in at.items()}
    order = [at[ys[0], z] for z in zs]
    for step, z in enumerate(reversed(zs)):
        rest = ys[1:] if step % 2 == 0 else ys[:0:-1]
        order += [at[y, z] for y in rest]
    return order


def narrow_kernel(me_ref, whole_ref, factor_ref, low_ref, high_ref, out_ref):
    narrow = (whole_ref[...] / factor_ref[...]).astype(jnp.bfloat16)
    out_ref[...] = narrow
    half = pl.num_programs(0) // 2

    @pl.when(pl.program_id(0) < half)
    def _():
        low_ref[...] = narrow

    @pl.when(pl.program_id(0) >= half)
    def _():
        high_ref[...] = narrow


def narrowed(whole, factor, me, count):
    rows, width = whole.shape
    tile = rows // 4
    blocks = rows // tile
    half = blocks // 2
    part = jax.ShapeDtypeStruct((rows // 2, width), jnp.bfloat16)
    return pl.pallas_call(
        narrow_kernel,
        grid_spec=pltpu.PrefetchScalarGridSpec(
            num_scalar_prefetch=1,
            grid=(blocks,),
            in_specs=[
                pl.BlockSpec((tile, width), lambda i, me: (i, 0)),
                pl.BlockSpec((1, width), lambda i, me: (0, 0)),
            ],
            out_specs=[
                pl.BlockSpec((tile, width), lambda i, me: (jnp.minimum(i, half - 1), 0)),
                pl.BlockSpec((tile, width), lambda i, me: (jnp.maximum(i - half, 0), 0)),
                pl.BlockSpec((tile, width), lambda i, me: (me[0] * blocks + i, 0)),
            ],
        ),
        out_shape=[part, part, jax.ShapeDtypeStruct((rows * count, width), jnp.bfloat16)],
        cost_estimate=pl.CostEstimate(
            flops=rows * width, bytes_accessed=8 * rows * width, transcendentals=0
        ),
    )(me.reshape(1), whole, factor.reshape(1, width))


def solution(mesh):
    count = mesh.shape["rows"]
    order = cycle_of(mesh)
    spot = [0] * count
    for at, row in enumerate(order):
        spot[row] = at
    right = [(order[i], order[(i + 1) % count]) for i in range(count)]
    left = [(b, a) for a, b in right]

    def shards(
        train_gate, drift_gate, spread_gate, train_up, drift_up, spread_up, norm_train, norm_step
    ):
        rows = train_gate.shape[0]
        total_rows = rows * count
        half = rows // 2
        me = lax.axis_index("rows")
        mine = jnp.asarray(spot, jnp.int32)[me]
        order_of = jnp.asarray(order, jnp.int32)

        def step(train, drift, spread):
            whole = train - learn_rate * (hold_rate * drift + spread)
            total = lax.psum(jnp.sum(jnp.abs(whole), axis=0), "rows")
            factor = total / total_rows
            return whole, factor, narrowed(whole, factor, me, count)

        whole_gate, factor_gate, (low_gate, high_gate, out_gate) = step(
            train_gate, drift_gate, spread_gate
        )
        whole_up, factor_up, (low_up, high_up, out_up) = step(train_up, drift_up, spread_up)
        low, high, outs = [low_gate, low_up], [high_gate, high_up], [out_gate, out_up]
        for hop in range(1, count):
            before = order_of[lax.rem(mine - hop + count, count)] * rows
            after = order_of[lax.rem(mine + hop, count)] * rows + half
            for i in range(2):
                low[i] = lax.ppermute(low[i], "rows", right)
                high[i] = lax.ppermute(high[i], "rows", left)
                outs[i] = lax.dynamic_update_slice(outs[i], low[i], (before, 0))
                outs[i] = lax.dynamic_update_slice(outs[i], high[i], (after, 0))
        serve_norm = lax.all_gather(
            (norm_train + norm_step).astype(jnp.bfloat16), ("rows", "tp"), axis=0, tiled=True
        )
        return (outs[0], outs[1], factor_gate, factor_up, serve_norm, whole_gate, whole_up)

    part = P("rows", "tp")
    flat = P(("rows", "tp"))
    return jax.shard_map(
        shards,
        mesh=mesh,
        in_specs=(part,) * 6 + (flat, flat),
        out_specs=(P(None, "tp"), P(None, "tp"), P("tp"), P("tp"), P(), part, part),
        check_vma=False,
    )
```

```python
import functools

import jax
import jax.numpy as jnp
import numpy as np
from jax import lax
from jax.experimental import pallas as pl
from jax.experimental.pallas import tpu as pltpu
from jax.sharding import PartitionSpec as P


learn_rate = 0.3
hold_rate = 0.9


def cycle_of(mesh):
    count = mesh.shape["rows"]
    try:
        spots = [tuple(d.coords[1:]) for d in np.asarray(mesh.devices)[:, 0]]
    except (AttributeError, TypeError):
        return list(range(count))
    ys = sorted({s[0] for s in spots})
    zs = sorted({s[1] for s in spots})
    at = {s: i for i, s in enumerate(spots)}
    if len(at) != count or len(ys) * len(zs) != count:
        return list(range(count))
    if len(zs) % 2 and len(ys) % 2 == 0:
        ys, zs = zs, ys
        at = {(b, a): i for (a, b), i in at.items()}
    order = [at[ys[0], z] for z in zs]
    for step, z in enumerate(reversed(zs)):
        rest = ys[1:] if step % 2 == 0 else ys[:0:-1]
        order += [at[y, z] for y in rest]
    return order


def exchange_kernel(
    total_rows, gate_ref, up_ref, norm_ref, factor_gate, factor_up, norm_out,
    gates, ups, shared, norms, sum_send, sum_recv, tp_send, tp_recv, norm_send, norm_recv, own_sem
):
    count, width = gates.shape[0], shared.shape[0]
    row, col = lax.axis_index("rows"), lax.axis_index("tp")

    def send(src, dst, send_sem, recv_sem, axis, peer):
        return pltpu.make_async_remote_copy(
            src_ref=src,
            dst_ref=dst,
            send_sem=send_sem,
            recv_sem=recv_sem,
            device_id={axis: peer},
            device_id_type=pl.DeviceIdType.MESH,
        )

    barrier = pltpu.get_barrier_semaphore()
    for axis, me, size in (("rows", row, count), ("tp", col, width)):
        for k in range(1, size):
            pl.semaphore_signal(
                barrier,
                inc=1,
                device_id={axis: lax.rem(me + k, size)},
                device_id_type=pl.DeviceIdType.MESH,
            )
    pl.semaphore_wait(barrier, count + width - 2)

    def across(k, slot):
        peer = lax.rem(col + k, width)
        return send(norm_ref, shared.at[slot], tp_send.at[k], tp_recv.at[slot], "tp", peer)

    def sums(k, slot):
        peer = lax.rem(row + k, count)
        return [
            send(ref, all_of.at[slot], sum_send.at[i, k], sum_recv.at[i, slot], "rows", peer)
            for i, (ref, all_of) in enumerate(((gate_ref, gates), (up_ref, ups)))
        ]

    def along(k, slot):
        peer = lax.rem(row + k, count)
        return send(shared, norms.at[slot], norm_send.at[k], norm_recv.at[slot], "rows", peer)

    for k in range(1, width):
        across(k, col).start()
    for k in range(1, count):
        for copy in sums(k, row):
            copy.start()
    mine = pltpu.make_async_copy(norm_ref, shared.at[col], own_sem)
    mine.start()
    gates[row] = gate_ref[...]
    ups[row] = up_ref[...]
    mine.wait()
    for k in range(1, width):
        across(k, lax.rem(col + width - k, width)).wait_recv()
    for k in range(1, count):
        along(k, row).start()
    mine = pltpu.make_async_copy(shared, norms.at[row], own_sem)
    mine.start()
    for k in range(1, count):
        for copy in sums(k, lax.rem(row + count - k, count)):
            copy.wait_recv()
    factor_gate[...] = jnp.sum(gates[...], axis=0) / total_rows
    factor_up[...] = jnp.sum(ups[...], axis=0) / total_rows
    mine.wait()
    for k in range(1, count):
        along(k, lax.rem(row + count - k, count)).wait_recv()
    norm_out[...] = norms[...]
    for k in range(1, width):
        across(k, col).wait_send()
    for k in range(1, count):
        along(k, row).wait_send()
        for copy in sums(k, row):
            copy.wait_send()


def exchanged(gate, up, norm, total_rows, count, width):
    share = norm.shape[0]
    lines = -(-share // 1024) * 8
    norm = jnp.pad(norm, (0, lines * 128 - share)).reshape(lines, 128)
    line = jax.ShapeDtypeStruct(gate.shape, jnp.float32)
    block = (lines, 128)
    dma = pltpu.SemaphoreType.DMA
    vmem = pl.BlockSpec(memory_space=pltpu.VMEM)
    factor_gate, factor_up, norms = pl.pallas_call(
        functools.partial(exchange_kernel, total_rows),
        out_shape=[line, line, jax.ShapeDtypeStruct((count, width) + block, jnp.float32)],
        in_specs=[vmem] * 3,
        out_specs=[vmem] * 3,
        scratch_shapes=[
            pltpu.VMEM((count,) + gate.shape, jnp.float32),
            pltpu.VMEM((count,) + gate.shape, jnp.float32),
            pltpu.VMEM((width,) + block, jnp.float32),
            pltpu.VMEM((count, width) + block, jnp.float32),
            dma((2, count)),
            dma((2, count)),
            dma((width,)),
            dma((width,)),
            dma((count,)),
            dma((count,)),
            dma,
        ],
        compiler_params=pltpu.CompilerParams(collective_id=0, has_side_effects=True),
    )(gate, up, norm)
    norms = norms.reshape(count * width, -1)[:, :share].reshape(-1)
    return factor_gate, factor_up, norms.astype(jnp.bfloat16)


def narrow_kernel(me_ref, whole_ref, factor_ref, low_ref, high_ref, out_ref):
    narrow = (whole_ref[...] / factor_ref[...]).astype(jnp.bfloat16)
    out_ref[...] = narrow
    half = pl.num_programs(0) // 2

    @pl.when(pl.program_id(0) < half)
    def _():
        low_ref[...] = narrow

    @pl.when(pl.program_id(0) >= half)
    def _():
        high_ref[...] = narrow


def narrowed(whole, factor, me, count):
    rows, width = whole.shape
    tile = rows // 4
    blocks = rows // tile
    half = blocks // 2
    part = jax.ShapeDtypeStruct((rows // 2, width), jnp.bfloat16)
    return pl.pallas_call(
        narrow_kernel,
        grid_spec=pltpu.PrefetchScalarGridSpec(
            num_scalar_prefetch=1,
            grid=(blocks,),
            in_specs=[
                pl.BlockSpec((tile, width), lambda i, me: (i, 0)),
                pl.BlockSpec((1, width), lambda i, me: (0, 0)),
            ],
            out_specs=[
                pl.BlockSpec((tile, width), lambda i, me: (jnp.minimum(i, half - 1), 0)),
                pl.BlockSpec((tile, width), lambda i, me: (jnp.maximum(i - half, 0), 0)),
                pl.BlockSpec((tile, width), lambda i, me: (me[0] * blocks + i, 0)),
            ],
        ),
        out_shape=[part, part, jax.ShapeDtypeStruct((rows * count, width), jnp.bfloat16)],
        cost_estimate=pl.CostEstimate(
            flops=rows * width, bytes_accessed=8 * rows * width, transcendentals=0
        ),
    )(me.reshape(1), whole, factor)


def solution(mesh):
    count = mesh.shape["rows"]
    order = cycle_of(mesh)
    spot = [0] * count
    for at, row in enumerate(order):
        spot[row] = at
    right = [(order[i], order[(i + 1) % count]) for i in range(count)]
    left = [(b, a) for a, b in right]

    def shards(
        train_gate, drift_gate, spread_gate, train_up, drift_up, spread_up, norm_train, norm_step
    ):
        rows = train_gate.shape[0]
        total_rows = rows * count
        half = rows // 2
        me = lax.axis_index("rows")
        mine = jnp.asarray(spot, jnp.int32)[me]
        order_of = jnp.asarray(order, jnp.int32)

        def step(train, drift, spread):
            whole = train - learn_rate * (hold_rate * drift + spread)
            return whole, jnp.sum(jnp.abs(whole), axis=0, keepdims=True)

        whole_gate, total_gate = step(train_gate, drift_gate, spread_gate)
        whole_up, total_up = step(train_up, drift_up, spread_up)
        factor_gate, factor_up, serve_norm = exchanged(
            total_gate, total_up, norm_train + norm_step, total_rows, count, mesh.shape["tp"]
        )
        low_gate, high_gate, out_gate = narrowed(whole_gate, factor_gate, me, count)
        low_up, high_up, out_up = narrowed(whole_up, factor_up, me, count)
        low, high, outs = [low_gate, low_up], [high_gate, high_up], [out_gate, out_up]
        for hop in range(1, count):
            before = order_of[lax.rem(mine - hop + count, count)] * rows
            after = order_of[lax.rem(mine + hop, count)] * rows + half
            for i in range(2):
                low[i] = lax.ppermute(low[i], "rows", right)
                high[i] = lax.ppermute(high[i], "rows", left)
                outs[i] = lax.dynamic_update_slice(outs[i], low[i], (before, 0))
                outs[i] = lax.dynamic_update_slice(outs[i], high[i], (after, 0))
        factor_gate, factor_up = factor_gate.reshape(-1), factor_up.reshape(-1)
        return (outs[0], outs[1], factor_gate, factor_up, serve_norm, whole_gate, whole_up)

    part = P("rows", "tp")
    flat = P(("rows", "tp"))
    return jax.shard_map(
        shards,
        mesh=mesh,
        in_specs=(part,) * 6 + (flat, flat),
        out_specs=(P(None, "tp"), P(None, "tp"), P("tp"), P("tp"), P(), part, part),
        check_vma=False,
    )
```

```python
import functools

import jax
import jax.numpy as jnp
import numpy as np
from jax import lax
from jax.experimental import pallas as pl
from jax.experimental.pallas import tpu as pltpu
from jax.sharding import PartitionSpec as P


learn_rate = 0.3
hold_rate = 0.9


def cycle_of(mesh):
    count = mesh.shape["rows"]
    try:
        spots = [tuple(d.coords[1:]) for d in np.asarray(mesh.devices)[:, 0]]
    except (AttributeError, TypeError):
        return list(range(count))
    ys = sorted({s[0] for s in spots})
    zs = sorted({s[1] for s in spots})
    at = {s: i for i, s in enumerate(spots)}
    if len(at) != count or len(ys) * len(zs) != count:
        return list(range(count))
    if len(zs) % 2 and len(ys) % 2 == 0:
        ys, zs = zs, ys
        at = {(b, a): i for (a, b), i in at.items()}
    order = [at[ys[0], z] for z in zs]
    for step, z in enumerate(reversed(zs)):
        rest = ys[1:] if step % 2 == 0 else ys[:0:-1]
        order += [at[y, z] for y in rest]
    return order


def moved(train_ref, drift_ref, spread_ref):
    return train_ref[...] - learn_rate * (hold_rate * drift_ref[...] + spread_ref[...])


def exchange_kernel(
    total_rows, train_gate, drift_gate, spread_gate, train_up, drift_up, spread_up,
    norm_train, norm_step, factor_gate, factor_up, norm_out,
    gate_acc, up_acc, gate_ref, up_ref, norm_ref, gates, ups, shared, norms,
    sum_send, sum_recv, tp_send, tp_recv, norm_send, norm_recv, own_sem
):
    count, width = gates.shape[0], shared.shape[0]
    row, col = lax.axis_index("rows"), lax.axis_index("tp")
    at, last = pl.program_id(0), pl.num_programs(0) - 1

    def send(src, dst, send_sem, recv_sem, axis, peer):
        return pltpu.make_async_remote_copy(
            src_ref=src,
            dst_ref=dst,
            send_sem=send_sem,
            recv_sem=recv_sem,
            device_id={axis: peer},
            device_id_type=pl.DeviceIdType.MESH,
        )

    def across(k, slot):
        peer = lax.rem(col + k, width)
        return send(norm_ref, shared.at[slot], tp_send.at[k], tp_recv.at[slot], "tp", peer)

    def sums(k, slot):
        peer = lax.rem(row + k, count)
        return [
            send(ref, all_of.at[slot], sum_send.at[i, k], sum_recv.at[i, slot], "rows", peer)
            for i, (ref, all_of) in enumerate(((gate_ref, gates), (up_ref, ups)))
        ]

    def along(k, slot):
        peer = lax.rem(row + k, count)
        return send(shared, norms.at[slot], norm_send.at[k], norm_recv.at[slot], "rows", peer)

    @pl.when(at == 0)
    def _():
        barrier = pltpu.get_barrier_semaphore()
        for axis, me, size in (("rows", row, count), ("tp", col, width)):
            for k in range(1, size):
                pl.semaphore_signal(
                    barrier,
                    inc=1,
                    device_id={axis: lax.rem(me + k, size)},
                    device_id_type=pl.DeviceIdType.MESH,
                )
        norm_ref[...] = jnp.zeros_like(norm_ref)
        norm_ref[:, : norm_train.shape[1]] = norm_train[...] + norm_step[...]
        gate_acc[...] = jnp.zeros_like(gate_acc)
        up_acc[...] = jnp.zeros_like(up_acc)

    for acc, refs in (
        (gate_acc, (train_gate, drift_gate, spread_gate)),
        (up_acc, (train_up, drift_up, spread_up)),
    ):
        size = jnp.abs(moved(*refs))
        acc[...] += jnp.sum(size.reshape((-1,) + acc.shape), axis=0)

    @pl.when(at == 1)
    def _():
        barrier = pltpu.get_barrier_semaphore()
        pl.semaphore_wait(barrier, count + width - 2)
        for k in range(1, width):
            across(k, col).start()
        mine = pltpu.make_async_copy(norm_ref, shared.at[col], own_sem)
        mine.start()
        mine.wait()

    @pl.when(at == last // 2 + 1)
    def _():
        for k in range(1, width):
            across(k, lax.rem(col + width - k, width)).wait_recv()
        for k in range(1, count):
            along(k, row).start()
        mine = pltpu.make_async_copy(shared, norms.at[row], own_sem)
        mine.start()
        mine.wait()

    @pl.when(at == last)
    def _():
        gate_ref[...] = jnp.sum(gate_acc[...], axis=0, keepdims=True)
        up_ref[...] = jnp.sum(up_acc[...], axis=0, keepdims=True)
        gates[row] = gate_ref[...]
        ups[row] = up_ref[...]
        for k in range(1, count):
            for copy in sums(k, row):
                copy.start()
        for k in range(1, count):
            along(k, lax.rem(row + count - k, count)).wait_recv()
        norm_out[...] = norms[...]
        for k in range(1, width):
            across(k, col).wait_send()
        for k in range(1, count):
            along(k, row).wait_send()
        for k in range(1, count):
            for copy in sums(k, lax.rem(row + count - k, count)):
                copy.wait_recv()
        factor_gate[...] = jnp.sum(gates[...], axis=0) / total_rows
        factor_up[...] = jnp.sum(ups[...], axis=0) / total_rows
        for k in range(1, count):
            for copy in sums(k, row):
                copy.wait_send()


def exchanged(gate, up, norm, total_rows, count, width):
    share = norm[0].shape[0]
    lanes = -(-share // 128) * 128
    rows, columns = gate[0].shape
    tile = rows // 8
    line = jax.ShapeDtypeStruct((1, columns), jnp.float32)
    block = (1, lanes)
    dma = pltpu.SemaphoreType.DMA
    vmem = pl.BlockSpec(memory_space=pltpu.VMEM)
    factor_gate, factor_up, norms = pl.pallas_call(
        functools.partial(exchange_kernel, total_rows),
        grid=(rows // tile,),
        out_shape=[line, line, jax.ShapeDtypeStruct((count, width) + block, jnp.float32)],
        in_specs=[pl.BlockSpec((tile, columns), lambda i: (i, 0))] * 6 + [vmem] * 2,
        out_specs=[vmem] * 3,
        scratch_shapes=[
            pltpu.VMEM((8, columns), jnp.float32),
            pltpu.VMEM((8, columns), jnp.float32),
            pltpu.VMEM((1, columns), jnp.float32),
            pltpu.VMEM((1, columns), jnp.float32),
            pltpu.VMEM(block, jnp.float32),
            pltpu.VMEM((count, 1, columns), jnp.float32),
            pltpu.VMEM((count, 1, columns), jnp.float32),
            pltpu.VMEM((width,) + block, jnp.float32),
            pltpu.VMEM((count, width) + block, jnp.float32),
            dma((2, count)),
            dma((2, count)),
            dma((width,)),
            dma((width,)),
            dma((count,)),
            dma((count,)),
            dma,
        ],
        compiler_params=pltpu.CompilerParams(collective_id=0, has_side_effects=True),
    )(*gate, *up, *(part.reshape(1, share) for part in norm))
    norms = norms.reshape(count * width, lanes)[:, :share].reshape(-1)
    return factor_gate, factor_up, norms.astype(jnp.bfloat16)


def narrow_kernel(
    me_ref, train_ref, drift_ref, spread_ref, factor_ref,
    low_ref, high_ref, out_ref, whole_ref, scale_ref
):
    whole = moved(train_ref, drift_ref, spread_ref)
    whole_ref[...] = whole
    scale_ref[...] = factor_ref[...]
    narrow = (whole / factor_ref[...]).astype(jnp.bfloat16)
    out_ref[...] = narrow
    half = pl.num_programs(0) // 2

    @pl.when(pl.program_id(0) < half)
    def _():
        low_ref[...] = narrow

    @pl.when(pl.program_id(0) >= half)
    def _():
        high_ref[...] = narrow


def narrowed(arrays, factor, me, count):
    rows, width = arrays[0].shape
    tile = rows // 4
    blocks = rows // tile
    half = blocks // 2
    part = jax.ShapeDtypeStruct((rows // 2, width), jnp.bfloat16)
    return pl.pallas_call(
        narrow_kernel,
        grid_spec=pltpu.PrefetchScalarGridSpec(
            num_scalar_prefetch=1,
            grid=(blocks,),
            in_specs=[
                *[pl.BlockSpec((tile, width), lambda i, me: (i, 0))] * 3,
                pl.BlockSpec((1, width), lambda i, me: (0, 0)),
            ],
            out_specs=[
                pl.BlockSpec((tile, width), lambda i, me: (jnp.minimum(i, half - 1), 0)),
                pl.BlockSpec((tile, width), lambda i, me: (jnp.maximum(i - half, 0), 0)),
                pl.BlockSpec((tile, width), lambda i, me: (me[0] * blocks + i, 0)),
                pl.BlockSpec((tile, width), lambda i, me: (i, 0)),
                pl.BlockSpec((1, width), lambda i, me: (0, 0)),
            ],
        ),
        out_shape=[
            part,
            part,
            jax.ShapeDtypeStruct((rows * count, width), jnp.bfloat16),
            jax.ShapeDtypeStruct((rows, width), jnp.float32),
            jax.ShapeDtypeStruct((1, width), jnp.float32),
        ],
        cost_estimate=pl.CostEstimate(
            flops=rows * width, bytes_accessed=20 * rows * width, transcendentals=0
        ),
    )(me.reshape(1), *arrays, factor)


def solution(mesh):
    count = mesh.shape["rows"]
    order = cycle_of(mesh)
    spot = [0] * count
    for at, row in enumerate(order):
        spot[row] = at
    right = [(order[i], order[(i + 1) % count]) for i in range(count)]
    left = [(b, a) for a, b in right]

    def shards(
        train_gate, drift_gate, spread_gate, train_up, drift_up, spread_up, norm_train, norm_step
    ):
        rows = train_gate.shape[0]
        total_rows = rows * count
        half = rows // 2
        me = lax.axis_index("rows")
        mine = jnp.asarray(spot, jnp.int32)[me]
        order_of = jnp.asarray(order, jnp.int32)

        gate = (train_gate, drift_gate, spread_gate)
        up = (train_up, drift_up, spread_up)
        factor_gate, factor_up, serve_norm = exchanged(
            gate, up, (norm_train, norm_step), total_rows, count, mesh.shape["tp"]
        )
        low_gate, high_gate, out_gate, whole_gate, factor_gate = narrowed(
            gate, factor_gate, me, count
        )
        low_up, high_up, out_up, whole_up, factor_up = narrowed(up, factor_up, me, count)
        low, high, outs = [low_gate, low_up], [high_gate, high_up], [out_gate, out_up]
        for hop in range(1, count):
            before = order_of[lax.rem(mine - hop + count, count)] * rows
            after = order_of[lax.rem(mine + hop, count)] * rows + half
            for i in range(2):
                low[i] = lax.ppermute(low[i], "rows", right)
                high[i] = lax.ppermute(high[i], "rows", left)
                outs[i] = lax.dynamic_update_slice(outs[i], low[i], (before, 0))
                outs[i] = lax.dynamic_update_slice(outs[i], high[i], (after, 0))
        factor_gate, factor_up = factor_gate.reshape(-1), factor_up.reshape(-1)
        return (outs[0], outs[1], factor_gate, factor_up, serve_norm, whole_gate, whole_up)

    part = P("rows", "tp")
    flat = P(("rows", "tp"))
    return jax.shard_map(
        shards,
        mesh=mesh,
        in_specs=(part,) * 6 + (flat, flat),
        out_specs=(P(None, "tp"), P(None, "tp"), P("tp"), P("tp"), P(), part, part),
        check_vma=False,
    )
```
